32 devices in a mesh: row: 4 (over y, x), col: 8 (over z, core).
Axes of the slice: x: 2, y: 2, z: 4, core: 2. Of those that a mesh axis runs over, the one named last changes fastest.
Arguments:
- pair_rep: bfloat16 [96, 96, 128], P('row', 'col'), may hold values from -6 to 6
- pair_mask: int32 [96, 96], P('row', 'col'), may hold values 0 or 1
- proj_weight: bfloat16 [2, 5, 128, 128], replicated, may hold values from -0.5 to 0.5
- out_weight: bfloat16 [2, 128, 128], replicated, may hold values from -0.5 to 0.5
- norm_gain: float32 [2, 2, 128], replicated, may hold values from 0.25 to 1.75
- norm_bias: float32 [2, 2, 128], replicated, may hold values from -1.5 to 1.5
Outputs:
- pair_out: bfloat16 [96, 96, 128], P('row', 'col')
The draws below stay inside these ranges and needn't reach their ends.
Inputs may be any that keep to these rules, and one draw needn't show every extreme that they name: pair_mask holds only 0 and 1.
All inputs are finite; a program needn't handle non-finite values.
Results may differ from the reference program's by a relative error of at most 0.0095.
Values may be sent and summed in bfloat16 or wider, within the bound.
A program may use at most 64 MiB of HBM per device.

```python
import jax
import jax.numpy as jnp
from jax import lax

C = 128
NRES = 96


def touch_ends(values, stream_key, least, high):
    index_at = [jax.random.randint(jax.random.fold_in(stream_key, axis), (), 0, length) for axis, length in enumerate(values.shape)]
    widest = values.shape.index(max(values.shape))
    beside = index_at[:widest] + [(index_at[widest] + 1) % values.shape[widest]] + index_at[widest + 1:]
    return values.at[tuple(index_at)].set(least).at[tuple(beside)].set(high)


def steps_of(own_key, dims, cuts, low, high):
    def one(dim, parts):
        heights = jax.random.uniform(jax.random.fold_in(jax.random.fold_in(own_key, 6), dim), (parts,), jnp.float32, low / len(cuts), high / len(cuts))
        return jnp.repeat(jnp.exp(heights), dims[dim] // parts).reshape((-1,) + (1,) * (len(dims) - dim - 1))

    gain = one(*cuts[0])
    for cut in cuts[1:]:
        gain = gain * one(*cut)
    return gain


def normal_values(rng, shape, deviation, bound, cuts=(), kind=jnp.bfloat16):
    array = jax.random.normal(rng, shape, jnp.float32) * deviation
    if len(cuts) > 0:
        array = steps_of(rng, shape, cuts, -0.22, 0.18) * array
    return jnp.clip(array, min=-bound, max=bound).astype(kind)


def setup_inputs(seed: int = 0) -> dict:
    key_of = jax.random.split(jax.random.key(seed), 7)
    return {
        "pair_rep": normal_values(key_of[0], (NRES, NRES, C), 1.0, 6.0, ((0, 4), (1, 8))),
        "pair_mask": touch_ends((jax.random.randint(key_of[1], (NRES, NRES), 0, 8) < 7).astype(jnp.int32), jax.random.fold_in(key_of[1], 1), 0, 1),
        "proj_weight": normal_values(key_of[2], (2, 5, C, C), C ** -0.5, 0.5),
        "out_weight": normal_values(key_of[3], (2, C, C), C ** -0.5, 0.5),
        "norm_gain": jnp.clip(1.0 + 0.15 * jax.random.normal(key_of[4], (2, 2, C), jnp.float32), 0.25, 1.75),
        "norm_bias": normal_values(key_of[5], (2, 2, C), 0.3, 1.5, (), jnp.float32),
    }


epsilon = 1e-05

def layer_norm(values, gain_vec, bias_vec):
    average = lax.optimization_barrier(jnp.mean(values, axis=-1, keepdims=True))
    centred = values - average
    variance = lax.optimization_barrier(jnp.mean(centred * centred, axis=-1, keepdims=True))
    return centred * lax.rsqrt(variance + epsilon) * gain_vec + bias_vec

def projections(pair_rep, mask_float, proj_weight, norm_gain, norm_bias, layer_no):
    normed = layer_norm(pair_rep.astype(jnp.float32), norm_gain[layer_no, 0], norm_bias[layer_no, 0]).astype(jnp.bfloat16)
    flattened = normed.reshape(-1, C)
    products = [jnp.dot(flattened, proj_weight[layer_no, which], preferred_element_type=jnp.float32).reshape(pair_rep.shape) for which in range(5)]
    left_side = (jax.nn.sigmoid(products[0]) * products[1] * mask_float).astype(jnp.bfloat16)
    right_side = (jax.nn.sigmoid(products[2]) * products[3] * mask_float).astype(jnp.bfloat16)
    gate_value = jax.nn.sigmoid(products[4])
    return (left_side, right_side, gate_value)

def finish(pair_rep, triangle, gate_value, out_weight, norm_gain, norm_bias, layer_no):
    normed = layer_norm(triangle, norm_gain[layer_no, 1], norm_bias[layer_no, 1]).astype(jnp.bfloat16)
    projected = jnp.dot(normed.reshape(-1, C), out_weight[layer_no], preferred_element_type=jnp.float32).reshape(pair_rep.shape)
    return (pair_rep.astype(jnp.float32) + gate_value * projected).astype(jnp.bfloat16)

def reference(pair_rep, pair_mask, proj_weight, out_weight, norm_gain, norm_bias):
    mask_float = pair_mask.astype(jnp.float32)[..., None]
    left_side, right_side, gate_value = projections(pair_rep, mask_float, proj_weight, norm_gain, norm_bias, 0)
    triangle = jnp.einsum('ikc,jkc->ijc', left_side.astype(jnp.float32), right_side.astype(jnp.float32))
    pair_rep = finish(pair_rep, triangle, gate_value, out_weight, norm_gain, norm_bias, 0)
    left_side, right_side, gate_value = projections(pair_rep, mask_float, proj_weight, norm_gain, norm_bias, 1)
    triangle = jnp.einsum('kic,kjc->ijc', left_side.astype(jnp.float32), right_side.astype(jnp.float32))
    pair_rep = finish(pair_rep, triangle, gate_value, out_weight, norm_gain, norm_bias, 1)
    return pair_rep
```

```python
import jax
import jax.numpy as jnp
from jax import lax
from jax.experimental import pallas as pl
from jax.experimental.pallas import tpu as pltpu
from jax.sharding import PartitionSpec as P

epsilon = 1e-05


def scattered(term, extent, axis):
    whole = term(jnp.int32(0), extent * lax.axis_size(axis))
    return lax.psum_scatter(whole, axis, scatter_dimension=0, tiled=True)


def layer_norm(values, gain_vec, bias_vec):
    average = jnp.mean(values, axis=-1, keepdims=True)
    centred = values - average
    variance = jnp.mean(centred * centred, axis=-1, keepdims=True)
    return centred * lax.rsqrt(variance + epsilon) * gain_vec + bias_vec


def projections(pair_rep, mask_float, proj_weight, norm_gain, norm_bias, layer_no):
    channels = pair_rep.shape[2]
    normed = layer_norm(
        pair_rep.astype(jnp.float32), norm_gain[layer_no, 0], norm_bias[layer_no, 0]
    ).astype(jnp.bfloat16)
    flattened = normed.reshape(-1, channels)
    products = [
        jnp.dot(
            flattened, proj_weight[layer_no, which], preferred_element_type=jnp.float32
        ).reshape(pair_rep.shape)
        for which in range(5)
    ]
    left_side = (jax.nn.sigmoid(products[0]) * products[1] * mask_float).astype(jnp.bfloat16)
    right_side = (jax.nn.sigmoid(products[2]) * products[3] * mask_float).astype(jnp.bfloat16)
    gate_value = jax.nn.sigmoid(products[4])
    return (left_side, right_side, gate_value)


def finish(pair_rep, triangle, gate_value, out_weight, norm_gain, norm_bias, layer_no):
    channels = pair_rep.shape[2]
    normed = layer_norm(triangle, norm_gain[layer_no, 1], norm_bias[layer_no, 1]).astype(
        jnp.bfloat16
    )
    projected = jnp.dot(
        normed.reshape(-1, channels), out_weight[layer_no], preferred_element_type=jnp.float32
    ).reshape(pair_rep.shape)
    return (pair_rep.astype(jnp.float32) + gate_value * projected).astype(jnp.bfloat16)


def shards(pair_rep, pair_mask, proj_weight, out_weight, norm_gain, norm_bias):
    rows_dev, cols_dev, channels = pair_rep.shape
    mask_float = pair_mask.astype(jnp.float32)[..., None]
    left_side, right_side, gate_value = projections(
        pair_rep, mask_float, proj_weight, norm_gain, norm_bias, 0
    )
    right_all = lax.all_gather(right_side, "row", axis=0, tiled=True)

    def outgoing_term(first_idx, how_many):
        sliced = lax.dynamic_slice_in_dim(right_all, first_idx, how_many, 0)
        return jnp.einsum("jkc,ikc->jic", sliced, left_side, preferred_element_type=jnp.float32)

    triangle = scattered(outgoing_term, cols_dev, "col")
    triangle = jnp.transpose(triangle, (1, 0, 2))
    pair_rep = finish(pair_rep, triangle, gate_value, out_weight, norm_gain, norm_bias, 0)
    left_side, right_side, gate_value = projections(
        pair_rep, mask_float, proj_weight, norm_gain, norm_bias, 1
    )
    left_all = lax.all_gather(left_side, "col", axis=1, tiled=True)

    def incoming_term(first_idx, how_many):
        sliced = lax.dynamic_slice_in_dim(left_all, first_idx, how_many, 1)
        return jnp.einsum("kic,kjc->ijc", sliced, right_side, preferred_element_type=jnp.float32)

    triangle = scattered(incoming_term, rows_dev, "row")
    pair_rep = finish(pair_rep, triangle, gate_value, out_weight, norm_gain, norm_bias, 1)
    return pair_rep


def layer_norm_rows(values, gain_vec, bias_vec):
    average = jnp.mean(values, axis=-1, keepdims=True)
    centred = values - average
    variance = jnp.mean(centred * centred, axis=-1, keepdims=True)
    return centred * lax.rsqrt(variance + epsilon) * gain_vec + bias_vec


def swapped(arrays, wanted, width, lane):
    groups = lane.shape[1] // width
    steps = []
    m = groups // 2
    while m:
        steps.append(m)
        m //= 2
    memo = {}

    def level(n, a):
        if n == 0:
            return arrays.get(a)
        if (n, a) not in memo:
            m = steps[n - 1]
            low, high = level(n - 1, a & ~m), level(n - 1, a | m)
            if a & m:
                moved = None if low is None else pltpu.roll(low, (groups - m) * width, 1)
                kept, other = high, moved
                pick_kept = (lane // width) & m != 0
            else:
                moved = None if high is None else pltpu.roll(high, m * width, 1)
                kept, other = low, moved
                pick_kept = (lane // width) & m == 0
            if kept is None:
                memo[n, a] = other
            elif other is None:
                memo[n, a] = kept
            else:
                memo[n, a] = jnp.where(pick_kept, kept, other)
        return memo[n, a]

    return {a: level(len(steps), a) for a in wanted}


def make_kernel(n_row, n_col, rows, cols, channels):
    n_dev = n_row * n_col
    width = channels // n_dev
    span = cols * width
    n_i, n_j = n_row * rows, n_col * cols
    pitch = -(-cols // 8) * 8
    bf16, f32 = jnp.bfloat16, jnp.float32

    def kernel(
        pair_ref, mask_ref, proj_ref, out_w_ref, gain_ref, bias_ref, out_ref,
        flat, expanded, square, outbox, inbox, back_out, back_in,
        send_sem, recv_sem,
    ):
        me_row, me_col = lax.axis_index("row"), lax.axis_index("col")
        me = me_row * n_col + me_col
        barrier = pltpu.get_barrier_semaphore()

        def place(offset):
            other = lax.rem(me + offset, n_dev)
            return other, (other // n_col, lax.rem(other, n_col))

        def greet(offset, carry):
            pl.semaphore_signal(
                barrier, inc=1, device_id=place(offset)[1],
                device_id_type=pl.DeviceIdType.MESH,
            )
            return carry

        lax.fori_loop(1, n_dev, greet, 0)

        def copy(source, target, phase, offset):
            other, where = place(offset)
            return pltpu.make_async_remote_copy(
                src_ref=source.at[other], dst_ref=target.at[me],
                send_sem=send_sem.at[phase, other], recv_sem=recv_sem.at[phase, me],
                device_id=where, device_id_type=pl.DeviceIdType.MESH,
            )

        def arrival(source, target, phase, offset):
            other, where = place(offset)
            return pltpu.make_async_remote_copy(
                src_ref=source.at[other], dst_ref=target.at[other],
                send_sem=send_sem.at[phase, other], recv_sem=recv_sem.at[phase, other],
                device_id=where, device_id_type=pl.DeviceIdType.MESH,
            )

        def exchange(source, target, phase):
            target[pl.ds(me, 1)] = source[pl.ds(me, 1)]

            def send(offset, carry):
                copy(source, target, phase, offset).start()
                return carry

            def receive(offset, carry):
                arrival(source, target, phase, offset).wait_recv()
                return carry

            lax.fori_loop(1, n_dev, send, 0)
            lax.fori_loop(1, n_dev, receive, 0)

        lane = lax.broadcasted_iota(jnp.int32, (rows, channels), 1)
        tall_lane = lax.broadcasted_iota(jnp.int32, (n_i, channels), 1)
        mask_float = mask_ref[...].astype(f32)

        for i in range(rows):
            flat[pitch * i : pitch * i + cols, :] = pair_ref[i].astype(f32)
        z = jnp.concatenate(
            [flat[pl.ds(j, rows, stride=pitch), :] for j in range(cols)], axis=0
        )

        for update in range(2):
            normed = layer_norm_rows(
                z, gain_ref[update, 0:1, :], bias_ref[update, 0:1, :]
            ).astype(bf16)
            products = [
                jnp.dot(normed, proj_ref[update, which], preferred_element_type=f32)
                for which in range(5)
            ]
            sides = {}
            for side in range(2):
                values = jax.nn.sigmoid(products[2 * side]) * products[2 * side + 1]
                for k in range(cols):
                    sides[side * cols + k] = (
                        values[k * rows : (k + 1) * rows, :] * mask_float[:, k : k + 1]
                    )
            gate_value = jax.nn.sigmoid(products[4])
            parcels = swapped(sides, range(n_dev), width, lane)
            for d in range(n_dev):
                outbox[update, d] = parcels[d].astype(bf16)
            if update == 0:
                pl.semaphore_wait(barrier, n_dev - 1)
            exchange(outbox.at[update], inbox.at[update], 2 * update)

            blocks = [
                jnp.concatenate(
                    [inbox[update, r * n_col + c].astype(f32) for r in range(n_row)], axis=0
                )
                for c in range(n_col)
            ]
            if update == 0:
                for c in range(n_col):
                    moved = pltpu.roll(blocks[c], channels - span, 1)
                    for q in range(width):
                        expanded[c, pl.ds(q, n_i, stride=width), :] = jnp.where(
                            (tall_lane < span) & (tall_lane % width == q), moved, 0.0
                        )
                triangle = lax.dot_general(
                    jnp.concatenate(blocks, axis=1).astype(bf16),
                    jnp.concatenate([expanded[c] for c in range(n_col)], axis=1).astype(bf16),
                    (((1,), (1,)), ((), ())),
                    preferred_element_type=f32,
                )
            else:
                lefts = jnp.concatenate([b[:, :span] for b in blocks], axis=1)
                rights = jnp.concatenate([b[:, span : 2 * span] for b in blocks], axis=1)
                whole = jnp.dot(
                    lefts.T.astype(bf16), rights.astype(bf16), preferred_element_type=f32
                )
                pieces = []
                for g in range(n_j * width // channels):
                    square[g] = whole[:, g * channels : (g + 1) * channels]
                    piece = square[g, pl.ds(0, n_i, stride=width), :]
                    for q in range(1, width):
                        piece = jnp.where(
                            tall_lane % width == q,
                            square[g, pl.ds(q, n_i, stride=width), :],
                            piece,
                        )
                    pieces.append(piece)
                triangle = jnp.concatenate(pieces, axis=1)
            for c in range(n_col):
                part = triangle[:, c * span : (c + 1) * span]
                for r in range(n_row):
                    back_out[update, r * n_col + c, :, :span] = (
                        part[r * rows : (r + 1) * rows, :].astype(bf16)
                    )
            exchange(back_out.at[update], back_in.at[update], 2 * update + 1)

            sums = swapped(
                {d: back_in[update, d].astype(f32) for d in range(n_dev)},
                range(cols), width, lane,
            )
            own = jnp.concatenate([sums[j] for j in range(cols)], axis=0)
            tnorm = layer_norm_rows(
                own, gain_ref[update, 1:2, :], bias_ref[update, 1:2, :]
            ).astype(bf16)
            projected = jnp.dot(tnorm, out_w_ref[update], preferred_element_type=f32)
            z = (z + gate_value * projected).astype(bf16).astype(f32)

        for j in range(cols):
            flat[pl.ds(j, rows, stride=pitch), :] = z[j * rows : (j + 1) * rows, :]
        for i in range(rows):
            out_ref[i] = flat[pitch * i : pitch * i + cols, :].astype(bf16)

        def sent(offset, carry):
            for update in range(2):
                copy(outbox.at[update], inbox.at[update], 2 * update, offset).wait_send()
                copy(back_out.at[update], back_in.at[update], 2 * update + 1, offset).wait_send()
            return carry

        lax.fori_loop(1, n_dev, sent, 0)

    parcel = pltpu.VMEM((2, n_dev, rows, channels), bf16)
    return pl.pallas_call(
        kernel,
        out_shape=jax.ShapeDtypeStruct((rows, cols, channels), bf16),
        in_specs=[pl.BlockSpec(memory_space=pltpu.VMEM)] * 6,
        out_specs=pl.BlockSpec(memory_space=pltpu.VMEM),
        scratch_shapes=[
            pltpu.VMEM((rows * pitch, channels), f32),
            pltpu.VMEM((n_col, n_j * width, channels), f32),
            pltpu.VMEM((n_j * width // channels, n_i * width, channels), f32),
            parcel, parcel, parcel, parcel,
            pltpu.SemaphoreType.DMA((4, n_dev)),
            pltpu.SemaphoreType.DMA((4, n_dev)),
        ],
        compiler_params=pltpu.CompilerParams(collective_id=0, has_side_effects=True),
    )


def solution(mesh):
    n_row, n_col = mesh.shape["row"], mesh.shape["col"]
    n_dev = n_row * n_col

    def local(pair_rep, *others):
        rows, cols, channels = pair_rep.shape
        by_channel = (
            channels == 128
            and channels % n_dev == 0
            and n_dev & (n_dev - 1) == 0
            and 2 * cols <= n_dev
            and rows % 8 == 0
            and n_row * rows == n_col * cols
            and n_col * cols * (channels // n_dev) % channels == 0
        )
        if by_channel:
            return make_kernel(n_row, n_col, rows, cols, channels)(pair_rep, *others)
        return shards(pair_rep, *others)

    in_specs = (P("row", "col", None), P("row", "col"), P(), P(), P(), P())
    out_specs = P("row", "col", None)
    return jax.shard_map(local, mesh=mesh, in_specs=in_specs, out_specs=out_specs, check_vma=False)
```

```python
import jax
import jax.numpy as jnp
from jax import lax
from jax.experimental import pallas as pl
from jax.experimental.pallas import tpu as pltpu
from jax.sharding import PartitionSpec as P

epsilon = 1e-05


def scattered(term, extent, axis):
    whole = term(jnp.int32(0), extent * lax.axis_size(axis))
    return lax.psum_scatter(whole, axis, scatter_dimension=0, tiled=True)


def layer_norm(values, gain_vec, bias_vec):
    average = jnp.mean(values, axis=-1, keepdims=True)
    centred = values - average
    variance = jnp.mean(centred * centred, axis=-1, keepdims=True)
    return centred * lax.rsqrt(variance + epsilon) * gain_vec + bias_vec


def projections(pair_rep, mask_float, proj_weight, norm_gain, norm_bias, layer_no):
    channels = pair_rep.shape[2]
    normed = layer_norm(
        pair_rep.astype(jnp.float32), norm_gain[layer_no, 0], norm_bias[layer_no, 0]
    ).astype(jnp.bfloat16)
    flattened = normed.reshape(-1, channels)
    products = [
        jnp.dot(
            flattened, proj_weight[layer_no, which], preferred_element_type=jnp.float32
        ).reshape(pair_rep.shape)
        for which in range(5)
    ]
    left_side = (jax.nn.sigmoid(products[0]) * products[1] * mask_float).astype(jnp.bfloat16)
    right_side = (jax.nn.sigmoid(products[2]) * products[3] * mask_float).astype(jnp.bfloat16)
    gate_value = jax.nn.sigmoid(products[4])
    return (left_side, right_side, gate_value)


def finish(pair_rep, triangle, gate_value, out_weight, norm_gain, norm_bias, layer_no):
    channels = pair_rep.shape[2]
    normed = layer_norm(triangle, norm_gain[layer_no, 1], norm_bias[layer_no, 1]).astype(
        jnp.bfloat16
    )
    projected = jnp.dot(
        normed.reshape(-1, channels), out_weight[layer_no], preferred_element_type=jnp.float32
    ).reshape(pair_rep.shape)
    return (pair_rep.astype(jnp.float32) + gate_value * projected).astype(jnp.bfloat16)


def shards(pair_rep, pair_mask, proj_weight, out_weight, norm_gain, norm_bias):
    rows_dev, cols_dev, channels = pair_rep.shape
    mask_float = pair_mask.astype(jnp.float32)[..., None]
    left_side, right_side, gate_value = projections(
        pair_rep, mask_float, proj_weight, norm_gain, norm_bias, 0
    )
    right_all = lax.all_gather(right_side, "row", axis=0, tiled=True)

    def outgoing_term(first_idx, how_many):
        sliced = lax.dynamic_slice_in_dim(right_all, first_idx, how_many, 0)
        return jnp.einsum("jkc,ikc->jic", sliced, left_side, preferred_element_type=jnp.float32)

    triangle = scattered(outgoing_term, cols_dev, "col")
    triangle = jnp.transpose(triangle, (1, 0, 2))
    pair_rep = finish(pair_rep, triangle, gate_value, out_weight, norm_gain, norm_bias, 0)
    left_side, right_side, gate_value = projections(
        pair_rep, mask_float, proj_weight, norm_gain, norm_bias, 1
    )
    left_all = lax.all_gather(left_side, "col", axis=1, tiled=True)

    def incoming_term(first_idx, how_many):
        sliced = lax.dynamic_slice_in_dim(left_all, first_idx, how_many, 1)
        return jnp.einsum("kic,kjc->ijc", sliced, right_side, preferred_element_type=jnp.float32)

    triangle = scattered(incoming_term, rows_dev, "row")
    pair_rep = finish(pair_rep, triangle, gate_value, out_weight, norm_gain, norm_bias, 1)
    return pair_rep


def layer_norm_rows(values, gain_vec, bias_vec):
    average = jnp.mean(values, axis=-1, keepdims=True)
    centred = values - average
    variance = jnp.mean(centred * centred, axis=-1, keepdims=True)
    return centred * lax.rsqrt(variance + epsilon) * gain_vec + bias_vec


def swapped(arrays, wanted, width, lane):
    groups = lane.shape[1] // width
    steps = []
    m = groups // 2
    while m:
        steps.append(m)
        m //= 2
    memo = {}

    def level(n, a):
        if n == 0:
            return arrays.get(a)
        if (n, a) not in memo:
            m = steps[n - 1]
            low, high = level(n - 1, a & ~m), level(n - 1, a | m)
            if a & m:
                moved = None if low is None else pltpu.roll(low, (groups - m) * width, 1)
                kept, other = high, moved
                pick_kept = (lane // width) & m != 0
            else:
                moved = None if high is None else pltpu.roll(high, m * width, 1)
                kept, other = low, moved
                pick_kept = (lane // width) & m == 0
            if kept is None:
                memo[n, a] = other
            elif other is None:
                memo[n, a] = kept
            else:
                memo[n, a] = jnp.where(pick_kept, kept, other)
        return memo[n, a]

    return {a: level(len(steps), a) for a in wanted}


def make_kernel(n_row, n_col, rows, cols, channels):
    n_dev = n_row * n_col
    width = channels // n_dev
    span = cols * width
    n_i, n_j = n_row * rows, n_col * cols
    upper = -(-rows // 16) * 8
    bf16, f32 = jnp.bfloat16, jnp.float32

    def kernel(
        pair_ref, mask_ref, proj_ref, out_w_ref, gain_ref, bias_ref, out_ref,
        expanded, square, outbox, inbox, back_out, back_in,
        send_sem, recv_sem,
    ):
        me_row, me_col = lax.axis_index("row"), lax.axis_index("col")
        me = me_row * n_col + me_col
        barrier = pltpu.get_barrier_semaphore()

        def place(offset):
            other = lax.rem(me + offset, n_dev)
            return other, (other // n_col, lax.rem(other, n_col))

        def greet(offset, carry):
            pl.semaphore_signal(
                barrier, inc=1, device_id=place(offset)[1],
                device_id_type=pl.DeviceIdType.MESH,
            )
            return carry

        lax.fori_loop(1, n_dev, greet, 0)

        def copy(source, target, phase, offset):
            other, where = place(offset)
            return pltpu.make_async_remote_copy(
                src_ref=source.at[other], dst_ref=target.at[me],
                send_sem=send_sem.at[phase, other], recv_sem=recv_sem.at[phase, me],
                device_id=where, device_id_type=pl.DeviceIdType.MESH,
            )

        def arrival(source, target, phase, offset):
            other, where = place(offset)
            return pltpu.make_async_remote_copy(
                src_ref=source.at[other], dst_ref=target.at[other],
                send_sem=send_sem.at[phase, other], recv_sem=recv_sem.at[phase, other],
                device_id=where, device_id_type=pl.DeviceIdType.MESH,
            )

        def exchange(source, target, phase):
            target[pl.ds(me, 1)] = source[pl.ds(me, 1)]

            def send(offset, carry):
                copy(source, target, phase, offset).start()
                return carry

            def receive(offset, carry):
                arrival(source, target, phase, offset).wait_recv()
                return carry

            lax.fori_loop(1, n_dev, send, 0)
            lax.fori_loop(1, n_dev, receive, 0)

        lane = lax.broadcasted_iota(jnp.int32, (rows, channels), 1)
        tall_lane = lax.broadcasted_iota(jnp.int32, (n_i, channels), 1)
        mask_float = mask_ref[...].astype(f32).T

        z = jnp.concatenate([pair_ref[j].astype(f32) for j in range(cols)], axis=0)

        for update in range(2):
            normed = layer_norm_rows(
                z, gain_ref[update, 0:1, :], bias_ref[update, 0:1, :]
            ).astype(bf16)
            products = [
                jnp.dot(normed, proj_ref[update, which], preferred_element_type=f32)
                for which in range(5)
            ]
            sides = {}
            for side in range(2):
                values = jax.nn.sigmoid(products[2 * side]) * products[2 * side + 1]
                for k in range(cols):
                    sides[side * cols + k] = (
                        values[k * rows : (k + 1) * rows, :] * mask_float[:, k : k + 1]
                    )
            gate_value = jax.nn.sigmoid(products[4])
            parcels = swapped(sides, range(n_dev), width, lane)
            for d in range(n_dev):
                outbox[update, d] = parcels[d].astype(bf16)
            if update == 0:
                pl.semaphore_wait(barrier, n_dev - 1)
            exchange(outbox.at[update], inbox.at[update], 2 * update)

            blocks = [
                jnp.concatenate(
                    [inbox[update, r * n_col + c].astype(f32) for r in range(n_row)], axis=0
                )
                for c in range(n_col)
            ]
            if update == 0:
                for c in range(n_col):
                    moved = pltpu.roll(blocks[c], channels - span, 1)
                    for q in range(width):
                        expanded[c, pl.ds(q, n_i, stride=width), :] = jnp.where(
                            (tall_lane < span) & (tall_lane % width == q), moved, 0.0
                        )
                triangle = lax.dot_general(
                    jnp.concatenate(blocks, axis=1).astype(bf16),
                    jnp.concatenate([expanded[c] for c in range(n_col)], axis=1).astype(bf16),
                    (((1,), (1,)), ((), ())),
                    preferred_element_type=f32,
                )
            else:
                lefts = jnp.concatenate([b[:, :span] for b in blocks], axis=1)
                rights = jnp.concatenate([b[:, span : 2 * span] for b in blocks], axis=1)
                whole = jnp.dot(
                    lefts.T.astype(bf16), rights.astype(bf16), preferred_element_type=f32
                )
                pieces = []
                for g in range(n_j * width // channels):
                    square[g] = whole[:, g * channels : (g + 1) * channels]
                    piece = square[g, pl.ds(0, n_i, stride=width), :]
                    for q in range(1, width):
                        piece = jnp.where(
                            tall_lane % width == q,
                            square[g, pl.ds(q, n_i, stride=width), :],
                            piece,
                        )
                    pieces.append(piece)
                triangle = jnp.concatenate(pieces, axis=1)
            for c in range(n_col):
                part = triangle[:, c * span : (c + 1) * span]
                for r in range(n_row):
                    mine = part[r * rows : (r + 1) * rows, :].astype(bf16)
                    back_out[update, r * n_col + c, :, :span] = mine[:upper, :]
                    back_out[update, r * n_col + c, : rows - upper, span : 2 * span] = mine[upper:, :]
            exchange(back_out.at[update], back_in.at[update], 2 * update + 1)

            arrived = {}
            for d in range(n_dev):
                packed = back_in[update, d].astype(f32)
                arrived[d] = jnp.concatenate(
                    [packed, pltpu.roll(packed[: rows - upper], channels - span, 1)], axis=0
                )
            sums = swapped(
                arrived,
                range(cols), width, lane,
            )
            own = jnp.concatenate([sums[j] for j in range(cols)], axis=0)
            tnorm = layer_norm_rows(
                own, gain_ref[update, 1:2, :], bias_ref[update, 1:2, :]
            ).astype(bf16)
            projected = jnp.dot(tnorm, out_w_ref[update], preferred_element_type=f32)
            z = (z + gate_value * projected).astype(bf16).astype(f32)

        for j in range(cols):
            out_ref[j] = z[j * rows : (j + 1) * rows, :].astype(bf16)

        def sent(offset, carry):
            for update in range(2):
                copy(outbox.at[update], inbox.at[update], 2 * update, offset).wait_send()
                copy(back_out.at[update], back_in.at[update], 2 * update + 1, offset).wait_send()
            return carry

        lax.fori_loop(1, n_dev, sent, 0)

    parcel = pltpu.VMEM((2, n_dev, rows, channels), bf16)
    back = pltpu.VMEM((2, n_dev, upper, channels), bf16)
    return pl.pallas_call(
        kernel,
        out_shape=jax.ShapeDtypeStruct((cols, rows, channels), bf16),
        in_specs=[pl.BlockSpec(memory_space=pltpu.VMEM)] * 6,
        out_specs=pl.BlockSpec(memory_space=pltpu.VMEM),
        scratch_shapes=[
            pltpu.VMEM((n_col, n_j * width, channels), f32),
            pltpu.VMEM((n_j * width // channels, n_i * width, channels), f32),
            parcel, parcel, back, back,
            pltpu.SemaphoreType.DMA((4, n_dev)),
            pltpu.SemaphoreType.DMA((4, n_dev)),
        ],
        compiler_params=pltpu.CompilerParams(collective_id=0, has_side_effects=True),
    )


def solution(mesh):
    n_row, n_col = mesh.shape["row"], mesh.shape["col"]
    n_dev = n_row * n_col

    def local(pair_rep, pair_mask, *others):
        rows, cols, channels = pair_rep.shape
        by_channel = (
            channels == 128
            and channels % n_dev == 0
            and n_dev & (n_dev - 1) == 0
            and 2 * cols <= n_dev
            and rows % 8 == 0
            and n_row * rows == n_col * cols
            and n_col * cols * (channels // n_dev) % channels == 0
        )
        if by_channel:
            kernel = make_kernel(n_row, n_col, rows, cols, channels)
            result = kernel(jnp.transpose(pair_rep, (1, 0, 2)), pair_mask.T, *others)
            return jnp.transpose(result, (1, 0, 2))
        return shards(pair_rep, pair_mask, *others)

    in_specs = (P("row", "col", None), P("row", "col"), P(), P(), P(), P())
    out_specs = P("row", "col", None)
    return jax.shard_map(local, mesh=mesh, in_specs=in_specs, out_specs=out_specs, check_vma=False)
```
